32 devices in a mesh: groups: 2 (over x), wide: 16 (over z, y, core).
Axes of the slice: x: 2, y: 2, z: 4, core: 2. Of those that a mesh axis runs over, the one named last changes fastest.
Arguments:
- half_integrals: float32 [256, 512, 800], P(('groups', 'wide')), parts along dimension 0, may hold values from -40 to 40
- pair_list: int32 [256, 2], P('groups'), parts along dimension 0, may hold values from 0 to 199, as said below
- occupied_energy: float32 [400], P('groups'), parts along dimension 0, may hold values from -3 to -0.3
- virtual_orbitals: float32 [1600, 600], P('groups'), parts along dimension 0, may hold values from -0.21875 to 0.21875
- tile_order: int32 [64], replicated, may hold values from 0 to 63, each once
Outputs:
- transformed: float32 [256, 512, 600], P('groups', 'wide'), parts along dimension 0
- pair_rms: float32 [256], P('groups'), parts along dimension 0
The draws below stay inside these ranges and needn't reach their ends.
There are 2 independent parts, one for each index of `groups`. The reference program is written for one: setup_inputs(seed, part) draws one part's arguments, and reference() takes and returns one part's arrays. A program takes and returns all parts, laid end to end along the dimension named above; an argument that names none is the same for every part. Nothing has to cross between parts.
Inputs may be any that keep to these rules, and one draw needn't show every extreme that they name: `pair_list`: each row is a distinct pair (i, j) with i <= j.
All inputs are finite; a program needn't handle non-finite values.
Results may differ from the reference program's by a relative error of at most 0.00007.
Values sent between devices are 32-bit elements; how exact they have to be, the bound alone decides.
A program may use at most 128 MiB of HBM per device.

```python
import jax
import jax.numpy as jnp
from jax import lax

NOCC = 200
NBAS = 800
NVIRT = 600
S_WIN = 512
TILE_S = 8
PAIRS = 128
TILES = 64


def draw_half_integrals(key, part):
    scale_key = jax.random.fold_in(key, 11)
    base_key = jax.random.fold_in(key, 12)
    column_scale = jnp.exp(jax.random.uniform(scale_key, (S_WIN,), jnp.float32, jnp.log(0.3), jnp.log(3.0)))
    base = jnp.clip(jax.random.normal(base_key, (PAIRS, S_WIN, NBAS), jnp.float32), -6.0, 6.0)
    return (base * column_scale[None, :, None]).astype(jnp.float32)


def draw_pair_list(key, part):
    total = NOCC * (NOCC + 1) // 2
    chosen = jax.random.permutation(jax.random.fold_in(key, 21), total)[:PAIRS].astype(jnp.int32)
    orbital = jnp.arange(NOCC, dtype=jnp.int32)
    triangle = orbital * (orbital + 1) // 2
    second = jnp.sum((triangle[None, :] <= chosen[:, None]).astype(jnp.int32), axis=1) - 1
    first = chosen - jnp.take(triangle, second)
    return jnp.stack([first, second], axis=1).astype(jnp.int32)


def normal_values(own_key, shape, width, most, kind=jnp.bfloat16):
    values = jax.random.normal(own_key, shape, jnp.float32) * width
    return jnp.minimum(jnp.maximum(values, -most), most).astype(kind)


def setup_inputs(seed: int = 0, part: int = 0) -> dict:
    keys = jax.random.split(jax.random.key(seed), 6)
    part_keys = jax.random.split(jax.random.fold_in(keys[5], part), 6)
    return {
        "half_integrals": draw_half_integrals(jax.random.fold_in(jax.random.fold_in(keys[5], part), 71), part),
        "pair_list": draw_pair_list(jax.random.fold_in(jax.random.fold_in(keys[5], part), 71), part),
        "occupied_energy": jnp.clip(jax.random.uniform(part_keys[2], (NOCC,), jnp.float32, -3.0, -0.3), -3.0, -0.3),
        "virtual_orbitals": normal_values(part_keys[3], (NBAS, NVIRT), NBAS ** -0.5, 0.21875, jnp.float32),
        "tile_order": jax.random.permutation(keys[4], TILES).astype(jnp.int32),
    }


def reference(half_integrals, pair_list, occupied_energy, virtual_orbitals, tile_order):
    energy_sum = occupied_energy[pair_list[:, 0]] + occupied_energy[pair_list[:, 1]]
    weights = jnp.exp(0.3 * energy_sum).astype(jnp.float32)
    pair_count = half_integrals.shape[0]
    tiled = half_integrals.reshape(pair_count, TILES, TILE_S, NBAS)
    ordered = jnp.take(tiled, tile_order, axis=1).reshape(pair_count, S_WIN, NBAS)
    product = jnp.einsum('psr,ra->psa', ordered, virtual_orbitals, precision=lax.Precision.HIGHEST)
    transformed = product * weights[:, None, None]
    squares = lax.optimization_barrier(jnp.sum(transformed * transformed, axis=(1, 2)))
    pair_rms = jnp.sqrt(squares / (S_WIN * NVIRT) + 1e-06)
    return (transformed, pair_rms)
```

```python
import functools

import jax
import jax.numpy as jnp
from jax import lax
from jax.experimental import pallas as pl
from jax.experimental.pallas import tpu as pltpu
from jax.sharding import PartitionSpec as P

TILE_S = 8
LANES = 128
MESH = pl.DeviceIdType.MESH


def round_up(value, step):
    return (value + step - 1) // step * step


def split(value):
    high = value.astype(jnp.bfloat16)
    low = (value - high.astype(jnp.float32)).astype(jnp.bfloat16)
    return high, low


def prepare_kernel(
    order_ref, pair_ref, energy_ref, x_ref, w_ref, xs, w_high, w_low, scales,
    index_buf, turned, slot_of, sems,
):
    me = lax.axis_index("wide")
    step = pl.program_id(0)
    steps = pl.num_programs(0)
    pair_rows, basis, _ = x_ref.shape
    virtuals = w_ref.shape[1]
    deep = xs.shape[0]
    block_rows = TILE_S * pair_rows
    tiles = LANES // TILE_S
    side = lax.rem(step, 2)

    @pl.when(step == 0)
    def _():
        def invert(k, carry):
            slot_of[order_ref[k]] = k
            return carry

        lax.fori_loop(0, order_ref.shape[0], invert, 0)
        w_high[...] = jnp.zeros_like(w_high)
        w_low[...] = jnp.zeros_like(w_low)
        high, low = split(w_ref[...])
        w_high[:basis, :virtuals] = high
        w_low[:basis, :virtuals] = low
        my_rows = pl.ds(pl.multiple_of(me * pair_rows, pair_rows), pair_rows)
        orbitals = energy_ref.shape[1]
        orbital = lax.broadcasted_iota(jnp.int32, (pair_rows, orbitals), 1).astype(jnp.float32)
        energy = jnp.zeros((pair_rows, 1), jnp.float32)
        for k in range(2):
            line = pair_ref[k : k + 1, :].astype(jnp.float32)
            index_buf[...] = jnp.broadcast_to(line, (LANES, line.shape[1])).T
            hit = index_buf[my_rows, 0:1] == orbital
            energy = energy + jnp.sum(jnp.where(hit, energy_ref[...], 0.0), axis=1, keepdims=True)
        scales[...] = jnp.broadcast_to(jnp.exp(0.3 * energy), scales.shape)

    def copy(at, which, u):
        rows = pl.ds(pl.multiple_of(slot_of[at * tiles + u] * block_rows, block_rows), block_rows)
        return pltpu.make_async_copy(
            turned.at[which, :, pl.ds(u * block_rows, block_rows), :], xs.at[:, rows, :], sems.at[which, u]
        )

    @pl.when(step >= 2)
    def _():
        for u in range(tiles):
            copy(step - 2, side, u).wait()

    for p in range(pair_rows):
        for k in range(deep):
            size = min(LANES, basis - k * LANES)
            piece = x_ref[p, k * LANES : k * LANES + size, :]
            if size < LANES:
                piece = jnp.concatenate([piece, jnp.zeros((LANES - size, LANES), jnp.float32)], axis=0)
            turned[side, k, pl.ds(p, LANES, stride=pair_rows), :] = piece.T
    for u in range(tiles):
        copy(step, side, u).start()

    @pl.when(step == steps - 1)
    def _():
        for u in range(tiles):
            copy(step - 1, 1 - side, u).wait()
        for u in range(tiles):
            copy(step, side, u).wait()


def exchange_kernel(
    n, xs, w_high, w_low, scales, recv_main, recv_rest, sq_recv,
    x_buf, x_high, x_low, squares, sq_send, send_main, send_rest,
    x_sems, main_sems, rest_sems, main_recv_sems, rest_recv_sems,
    sq_sems, sq_recv_sems, own_sems,
):
    me = lax.axis_index("wide")
    _, span, pair_rows, full = send_main.shape
    rest = send_rest.shape[2] // span
    rows = span * pair_rows
    deep = xs.shape[0]
    plane = n // 4
    my_rows = pl.ds(pl.multiple_of(me * pair_rows, pair_rows), pair_rows)

    barrier = pltpu.get_barrier_semaphore()

    def greet(j, carry):
        pl.semaphore_signal(barrier, inc=1, device_id={"wide": lax.rem(me + j, n)}, device_id_type=MESH)
        return carry

    lax.fori_loop(1, n, greet, 0)

    sign = 1 - 2 * (me // (n // 2))
    my_plane = me // plane

    def place(c):
        other = lax.rem(my_plane + sign * (1 + c // plane) + 8, 4)
        return other * plane + lax.rem(me + c, plane)

    def fetch(c):
        source = pl.ds(pl.multiple_of(place(c) * rows, rows), rows)
        side = lax.rem(c, 2)
        return pltpu.make_async_copy(xs.at[:, source, :], x_buf.at[side], x_sems.at[side])

    fetch(0).start()
    squares[...] = jnp.zeros_like(squares)

    def remotes(c, owner):
        return (
            pltpu.make_async_remote_copy(
                src_ref=send_main.at[c], dst_ref=recv_main.at[:, my_rows, :],
                send_sem=main_sems.at[c], recv_sem=main_recv_sems.at[me],
                device_id={"wide": owner}, device_id_type=MESH,
            ),
            pltpu.make_async_remote_copy(
                src_ref=send_rest.at[c], dst_ref=recv_rest.at[my_rows, :],
                send_sem=rest_sems.at[c], recv_sem=rest_recv_sems.at[me],
                device_id={"wide": owner}, device_id_type=MESH,
            ),
        )

    def locals_(c):
        return (
            pltpu.make_async_copy(send_main.at[c], recv_main.at[:, my_rows, :], own_sems.at[0]),
            pltpu.make_async_copy(send_rest.at[c], recv_rest.at[my_rows, :], own_sems.at[1]),
        )

    def dispatch(c):
        owner = place(c)

        @pl.when(owner != me)
        def _():
            for copy in remotes(c, owner):
                copy.start()

        @pl.when(owner == me)
        def _():
            for copy in locals_(c):
                copy.start()

    lane = lax.broadcasted_iota(jnp.int32, (pair_rows, LANES), 1)

    def block(c, carry):
        @pl.when(c + 1 < n)
        def _():
            fetch(c + 1).start()

        fetch(c).wait()
        for k in range(deep):
            high, low = split(x_buf[lax.rem(c, 2), k])
            x_high[:, k * LANES : (k + 1) * LANES] = high
            x_low[:, k * LANES : (k + 1) * LANES] = low
        dot = functools.partial(jnp.dot, preferred_element_type=jnp.float32)
        small = dot(x_low[...], w_high[...]) + dot(x_high[...], w_low[...])
        product = (dot(x_high[...], w_high[...]) + small).reshape(span, pair_rows, -1) * scales[...][None]
        squares[...] = squares[...] + jnp.sum(product * product, axis=0)
        send_main[c] = product[:, :, :full]
        packed = [jnp.zeros((pair_rows, LANES), jnp.float32)] * (span * rest // LANES)
        for s in range(span):
            at, offset = divmod(s * rest, LANES)
            value = product[s, :, full:]
            if offset:
                value = pltpu.roll(value, offset, axis=1)
            if offset + rest > LANES:
                packed[at] = jnp.where(lane >= offset, value, packed[at])
                packed[at + 1] = jnp.where(lane < offset, value, packed[at + 1])
            else:
                packed[at] = jnp.where(lane >= offset, value, packed[at])
        for b, value in enumerate(packed):
            send_rest[c, :, b * LANES : (b + 1) * LANES] = value

        @pl.when(c == 0)
        def _():
            pl.semaphore_wait(barrier, n - 1)

        @pl.when(c > 0)
        def _():
            dispatch(c - 1)

        return carry

    lax.fori_loop(0, n, block, 0)
    dispatch(n - 1)
    total = squares[:, :LANES]
    for b in range(1, squares.shape[1] // LANES):
        total = total + squares[:, b * LANES : (b + 1) * LANES]
    sq_send[...] = total

    def sq_copy(src, dst, j):
        return pltpu.make_async_remote_copy(
            src_ref=sq_send, dst_ref=sq_recv.at[src],
            send_sem=sq_sems.at[j], recv_sem=sq_recv_sems.at[src],
            device_id={"wide": dst}, device_id_type=MESH,
        )

    for copy in remotes(0, place(0)):
        copy.wait_send()
    own_squares = pltpu.make_async_copy(sq_send, sq_recv.at[me], own_sems.at[2])
    own_squares.start()

    def send_squares(j, carry):
        sq_copy(me, lax.rem(me + j, n), j).start()
        return carry

    lax.fori_loop(1, n, send_squares, 0)
    own_squares.wait()

    def finish_sends(c, carry):
        owner = place(c)

        @pl.when(owner != me)
        def _():
            for copy in remotes(c, owner):
                copy.wait_send()

        @pl.when(owner == me)
        def _():
            for copy in locals_(c):
                copy.wait()

        return carry

    lax.fori_loop(1, n, finish_sends, 0)

    def finish(j, carry):
        src = lax.rem(me + j, n)
        rows = pl.ds(pl.multiple_of(src * pair_rows, pair_rows), pair_rows)
        pltpu.make_async_remote_copy(
            src_ref=send_main.at[0], dst_ref=recv_main.at[:, rows, :],
            send_sem=main_sems.at[0], recv_sem=main_recv_sems.at[src],
            device_id={"wide": src}, device_id_type=MESH,
        ).wait_recv()
        pltpu.make_async_remote_copy(
            src_ref=send_rest.at[0], dst_ref=recv_rest.at[rows, :],
            send_sem=rest_sems.at[0], recv_sem=rest_recv_sems.at[src],
            device_id={"wide": src}, device_id_type=MESH,
        ).wait_recv()
        sq_copy(src, src, j).wait_recv()
        sq_copy(me, src, j).wait_send()
        return carry

    lax.fori_loop(1, n, finish, 0)


def unpack_kernel(count, main_ref, rest_ref, sq_ref, out_ref, rms_ref, turned):
    group, pairs, full = main_ref.shape
    rest = out_ref.shape[1] - full
    step = pl.program_id(0)

    @pl.when(step == 0)
    def _():
        for b in range(rest_ref.shape[1] // LANES):
            turned[b * LANES : (b + 1) * LANES, :] = rest_ref[:, b * LANES : (b + 1) * LANES].T
        totals = jnp.sum(sq_ref[...].T, axis=0, keepdims=True)
        rms_ref[...] = jnp.sqrt(totals / count + 1e-06)

    for g in range(group):
        for b in range(full // LANES):
            out_ref[g, b * LANES : (b + 1) * LANES, :] = main_ref[g, :, b * LANES : (b + 1) * LANES].T
        start = pl.multiple_of((step * group + g) * rest, 8)
        out_ref[g, full:, :] = turned[pl.ds(start, rest), :]


def shards(n, half_integrals, pair_list, occupied_energy, virtual_orbitals, tile_order):
    pair_rows, columns, basis = half_integrals.shape
    virtuals = virtual_orbitals.shape[1]
    pairs = n * pair_rows
    span = columns // n
    deep = round_up(basis, LANES)
    broad = round_up(virtuals, LANES)
    full = virtuals // LANES * LANES
    rest = virtuals - full
    rows = span * pair_rows
    group = 4
    flops = 6 * pair_rows * columns * basis * virtuals
    vmem = pl.BlockSpec(memory_space=pltpu.VMEM)
    anywhere = pl.BlockSpec(memory_space=pl.ANY)

    def whole(*shape):
        return pl.BlockSpec(shape, lambda i: (0,) * len(shape))

    tiles = LANES // TILE_S
    xs, w_high, w_low, scales = pl.pallas_call(
        prepare_kernel,
        grid=(columns // LANES,),
        out_shape=(
            jax.ShapeDtypeStruct((deep // LANES, columns * pair_rows, LANES), jnp.float32),
            jax.ShapeDtypeStruct((deep, broad), jnp.bfloat16),
            jax.ShapeDtypeStruct((deep, broad), jnp.bfloat16),
            jax.ShapeDtypeStruct((pair_rows, broad), jnp.float32),
        ),
        in_specs=[
            pl.BlockSpec(memory_space=pltpu.SMEM),
            whole(2, pairs),
            whole(1, occupied_energy.shape[0]),
            pl.BlockSpec((pair_rows, basis, LANES), lambda i: (0, 0, i)),
            whole(basis, virtuals),
        ],
        out_specs=(anywhere, whole(deep, broad), whole(deep, broad), whole(pair_rows, broad)),
        scratch_shapes=[
            pltpu.VMEM((pairs, LANES), jnp.float32),
            pltpu.VMEM((2, deep // LANES, LANES * pair_rows, LANES), jnp.float32),
            pltpu.SMEM(tile_order.shape, jnp.int32),
            pltpu.SemaphoreType.DMA((2, tiles)),
        ],
        compiler_params=pltpu.CompilerParams(vmem_limit_bytes=54 * 1024 * 1024),
        name="prepare",
    )(tile_order, pair_list.T, occupied_energy.reshape(1, -1), jnp.swapaxes(half_integrals, 1, 2), virtual_orbitals)
    recv_main, recv_rest, sq_recv = pl.pallas_call(
        functools.partial(exchange_kernel, n),
        out_shape=(
            jax.ShapeDtypeStruct((span, pairs, full), jnp.float32),
            jax.ShapeDtypeStruct((pairs, span * rest), jnp.float32),
            jax.ShapeDtypeStruct((n, pair_rows, LANES), jnp.float32),
        ),
        in_specs=[anywhere, vmem, vmem, vmem],
        out_specs=(anywhere, anywhere, anywhere),
        scratch_shapes=[
            pltpu.VMEM((2, deep // LANES, rows, LANES), jnp.float32),
            pltpu.VMEM((rows, deep), jnp.bfloat16),
            pltpu.VMEM((rows, deep), jnp.bfloat16),
            pltpu.VMEM((pair_rows, broad), jnp.float32),
            pltpu.VMEM((pair_rows, LANES), jnp.float32),
            pltpu.VMEM((n, span, pair_rows, full), jnp.float32),
            pltpu.VMEM((n, pair_rows, span * rest), jnp.float32),
            pltpu.SemaphoreType.DMA((2,)),
            pltpu.SemaphoreType.DMA((n,)),
            pltpu.SemaphoreType.DMA((n,)),
            pltpu.SemaphoreType.DMA((n,)),
            pltpu.SemaphoreType.DMA((n,)),
            pltpu.SemaphoreType.DMA((n,)),
            pltpu.SemaphoreType.DMA((n,)),
            pltpu.SemaphoreType.DMA((3,)),
        ],
        compiler_params=pltpu.CompilerParams(
            collective_id=0, has_side_effects=True, vmem_limit_bytes=30 * 1024 * 1024
        ),
        cost_estimate=pl.CostEstimate(flops=flops, bytes_accessed=4 * half_integrals.size, transcendentals=0),
        name="exchange",
    )(xs, w_high, w_low, scales)
    out, rms = pl.pallas_call(
        functools.partial(unpack_kernel, columns * virtuals),
        grid=(span // group,),
        out_shape=(
            jax.ShapeDtypeStruct((span, virtuals, pairs), jnp.float32),
            jax.ShapeDtypeStruct((1, pairs), jnp.float32),
        ),
        in_specs=[
            pl.BlockSpec((group, pairs, full), lambda i: (i, 0, 0)),
            pl.BlockSpec((pairs, span * rest), lambda i: (0, 0)),
            pl.BlockSpec((pairs, LANES), lambda i: (0, 0)),
        ],
        out_specs=(
            pl.BlockSpec((group, virtuals, pairs), lambda i: (i, 0, 0)),
            pl.BlockSpec((1, pairs), lambda i: (0, 0)),
        ),
        scratch_shapes=[pltpu.VMEM((span * rest, pairs), jnp.float32)],
        compiler_params=pltpu.CompilerParams(vmem_limit_bytes=20 * 1024 * 1024),
        name="unpack",
    )(recv_main, recv_rest, sq_recv.reshape(pairs, LANES))
    return (jnp.transpose(out, (2, 0, 1)), rms.reshape(-1))


def solution(mesh):
    in_specs = (
        P(("groups", "wide"), None, None),
        P("groups", None),
        P("groups"),
        P("groups", None),
        P(),
    )
    out_specs = (P("groups", "wide", None), P("groups"))
    return jax.shard_map(
        functools.partial(shards, mesh.shape["wide"]),
        mesh=mesh, in_specs=in_specs, out_specs=out_specs, check_vma=False,
    )
```

```python
import functools

import jax
import jax.numpy as jnp
from jax import lax
from jax.experimental import pallas as pl
from jax.experimental.pallas import tpu as pltpu
from jax.sharding import PartitionSpec as P

TILE_S = 8
LANES = 128
MESH = pl.DeviceIdType.MESH


def round_up(value, step):
    return (value + step - 1) // step * step


def split(value):
    high = value.astype(jnp.bfloat16)
    low = (value - high.astype(jnp.float32)).astype(jnp.bfloat16)
    return high, low


def prepare_kernel(
    order_ref, pair_ref, energy_ref, x_ref, w_ref, xs, w_high, w_low, scales,
    index_buf, turned, slot_of, sems,
):
    me = lax.axis_index("wide")
    step = pl.program_id(0)
    steps = pl.num_programs(0)
    pair_rows, basis, _ = x_ref.shape
    virtuals = w_ref.shape[1]
    deep = xs.shape[0]
    block_rows = TILE_S * pair_rows
    tiles = LANES // TILE_S
    side = lax.rem(step, 2)

    @pl.when(step == 0)
    def _():
        def invert(k, carry):
            slot_of[order_ref[k]] = k
            return carry

        lax.fori_loop(0, order_ref.shape[0], invert, 0)
        w_high[...] = jnp.zeros_like(w_high)
        w_low[...] = jnp.zeros_like(w_low)
        high, low = split(w_ref[...])
        w_high[:basis, :virtuals] = high
        w_low[:basis, :virtuals] = low
        my_rows = pl.ds(pl.multiple_of(me * pair_rows, pair_rows), pair_rows)
        orbitals = energy_ref.shape[1]
        orbital = lax.broadcasted_iota(jnp.int32, (pair_rows, orbitals), 1).astype(jnp.float32)
        energy = jnp.zeros((pair_rows, 1), jnp.float32)
        for k in range(2):
            line = pair_ref[k : k + 1, :].astype(jnp.float32)
            index_buf[...] = jnp.broadcast_to(line, (LANES, line.shape[1])).T
            hit = index_buf[my_rows, 0:1] == orbital
            energy = energy + jnp.sum(jnp.where(hit, energy_ref[...], 0.0), axis=1, keepdims=True)
        scales[...] = jnp.broadcast_to(jnp.exp(0.3 * energy), scales.shape)

    def copy(at, which, u):
        rows = pl.ds(pl.multiple_of(slot_of[at * tiles + u] * block_rows, block_rows), block_rows)
        return pltpu.make_async_copy(
            turned.at[which, :, pl.ds(u * block_rows, block_rows), :], xs.at[:, rows, :], sems.at[which, u]
        )

    @pl.when(step >= 2)
    def _():
        for u in range(tiles):
            copy(step - 2, side, u).wait()

    for p in range(pair_rows):
        for k in range(deep):
            size = min(LANES, basis - k * LANES)
            piece = x_ref[p, k * LANES : k * LANES + size, :]
            if size < LANES:
                piece = jnp.concatenate([piece, jnp.zeros((LANES - size, LANES), jnp.float32)], axis=0)
            turned[side, k, pl.ds(p, LANES, stride=pair_rows), :] = piece.T
    for u in range(tiles):
        copy(step, side, u).start()

    @pl.when(step == steps - 1)
    def _():
        for u in range(tiles):
            copy(step - 1, 1 - side, u).wait()
        for u in range(tiles):
            copy(step, side, u).wait()


def exchange_kernel(
    n, xs, w_high, w_low, scales, recv_main, recv_rest, sq_recv,
    x_buf, x_high, x_low, squares, sq_send, send_main, send_rest,
    x_sems, main_sems, rest_sems, main_recv_sems, rest_recv_sems,
    sq_sems, sq_recv_sems, own_sems,
):
    me = lax.axis_index("wide")
    _, span, pair_rows, full = send_main.shape
    rest = send_rest.shape[2] // span
    rows = span * pair_rows
    deep = xs.shape[0]
    plane = n // 4
    my_rows = pl.ds(pl.multiple_of(me * pair_rows, pair_rows), pair_rows)

    barrier = pltpu.get_barrier_semaphore()

    def greet(j, carry):
        pl.semaphore_signal(barrier, inc=1, device_id={"wide": lax.rem(me + j, n)}, device_id_type=MESH)
        return carry

    lax.fori_loop(1, n, greet, 0)

    sign = 1 - 2 * (me // (n // 2))
    my_plane = me // plane

    def place(c):
        other = lax.rem(my_plane + sign * (1 + c // plane) + 8, 4)
        return other * plane + lax.rem(me + c, plane)

    def fetch(c):
        source = pl.ds(pl.multiple_of(place(c) * rows, rows), rows)
        side = lax.rem(c, 2)
        return pltpu.make_async_copy(xs.at[:, source, :], x_buf.at[side], x_sems.at[side])

    fetch(0).start()
    squares[...] = jnp.zeros_like(squares)

    def remotes(c, owner):
        return (
            pltpu.make_async_remote_copy(
                src_ref=send_main.at[c], dst_ref=recv_main.at[:, my_rows, :],
                send_sem=main_sems.at[c], recv_sem=main_recv_sems.at[me],
                device_id={"wide": owner}, device_id_type=MESH,
            ),
            pltpu.make_async_remote_copy(
                src_ref=send_rest.at[c], dst_ref=recv_rest.at[my_rows, :],
                send_sem=rest_sems.at[c], recv_sem=rest_recv_sems.at[me],
                device_id={"wide": owner}, device_id_type=MESH,
            ),
        )

    def locals_(c):
        return (
            pltpu.make_async_copy(send_main.at[c], recv_main.at[:, my_rows, :], own_sems.at[0]),
            pltpu.make_async_copy(send_rest.at[c], recv_rest.at[my_rows, :], own_sems.at[1]),
        )

    def dispatch(c):
        owner = place(c)

        @pl.when(owner != me)
        def _():
            for copy in remotes(c, owner):
                copy.start()

        @pl.when(owner == me)
        def _():
            for copy in locals_(c):
                copy.start()

    lane = lax.broadcasted_iota(jnp.int32, (pair_rows, LANES), 1)

    def block(c, carry):
        @pl.when(c + 1 < n)
        def _():
            fetch(c + 1).start()

        fetch(c).wait()
        for k in range(deep):
            high, low = split(x_buf[lax.rem(c, 2), k])
            x_high[:, k * LANES : (k + 1) * LANES] = high
            x_low[:, k * LANES : (k + 1) * LANES] = low

        @pl.when(c == 1)
        def _():
            pl.semaphore_wait(barrier, n - 1)

        @pl.when(c > 0)
        def _():
            dispatch(c - 1)

        dot = functools.partial(jnp.dot, preferred_element_type=jnp.float32)
        small = dot(x_low[...], w_high[...]) + dot(x_high[...], w_low[...])
        product = (dot(x_high[...], w_high[...]) + small).reshape(span, pair_rows, -1) * scales[...][None]
        squares[...] = squares[...] + jnp.sum(product * product, axis=0)
        send_main[c] = product[:, :, :full]
        packed = [jnp.zeros((pair_rows, LANES), jnp.float32)] * (span * rest // LANES)
        for s in range(span):
            at, offset = divmod(s * rest, LANES)
            value = product[s, :, full:]
            if offset:
                value = pltpu.roll(value, offset, axis=1)
            if offset + rest > LANES:
                packed[at] = jnp.where(lane >= offset, value, packed[at])
                packed[at + 1] = jnp.where(lane < offset, value, packed[at + 1])
            else:
                packed[at] = jnp.where(lane >= offset, value, packed[at])
        for b, value in enumerate(packed):
            send_rest[c, :, b * LANES : (b + 1) * LANES] = value

        return carry

    lax.fori_loop(0, n, block, 0)
    dispatch(n - 1)
    total = squares[:, :LANES]
    for b in range(1, squares.shape[1] // LANES):
        total = total + squares[:, b * LANES : (b + 1) * LANES]
    sq_send[...] = total

    def sq_copy(src, dst, j):
        return pltpu.make_async_remote_copy(
            src_ref=sq_send, dst_ref=sq_recv.at[src],
            send_sem=sq_sems.at[j], recv_sem=sq_recv_sems.at[src],
            device_id={"wide": dst}, device_id_type=MESH,
        )

    for copy in remotes(0, place(0)):
        copy.wait_send()
    own_squares = pltpu.make_async_copy(sq_send, sq_recv.at[me], own_sems.at[2])
    own_squares.start()

    def send_squares(j, carry):
        sq_copy(me, lax.rem(me + j, n), j).start()
        return carry

    lax.fori_loop(1, n, send_squares, 0)
    own_squares.wait()

    def finish_sends(c, carry):
        owner = place(c)

        @pl.when(owner != me)
        def _():
            for copy in remotes(c, owner):
                copy.wait_send()

        @pl.when(owner == me)
        def _():
            for copy in locals_(c):
                copy.wait()

        return carry

    lax.fori_loop(1, n, finish_sends, 0)

    def finish(j, carry):
        src = lax.rem(me + j, n)
        rows = pl.ds(pl.multiple_of(src * pair_rows, pair_rows), pair_rows)
        pltpu.make_async_remote_copy(
            src_ref=send_main.at[0], dst_ref=recv_main.at[:, rows, :],
            send_sem=main_sems.at[0], recv_sem=main_recv_sems.at[src],
            device_id={"wide": src}, device_id_type=MESH,
        ).wait_recv()
        pltpu.make_async_remote_copy(
            src_ref=send_rest.at[0], dst_ref=recv_rest.at[rows, :],
            send_sem=rest_sems.at[0], recv_sem=rest_recv_sems.at[src],
            device_id={"wide": src}, device_id_type=MESH,
        ).wait_recv()
        sq_copy(src, src, j).wait_recv()
        sq_copy(me, src, j).wait_send()
        return carry

    lax.fori_loop(1, n, finish, 0)


def unpack_kernel(count, main_ref, rest_ref, sq_ref, out_ref, rms_ref, turned):
    group, pairs, full = main_ref.shape
    rest = out_ref.shape[1] - full
    step = pl.program_id(0)

    @pl.when(step == 0)
    def _():
        for b in range(rest_ref.shape[1] // LANES):
            turned[b * LANES : (b + 1) * LANES, :] = rest_ref[:, b * LANES : (b + 1) * LANES].T
        totals = jnp.sum(sq_ref[...].T, axis=0, keepdims=True)
        rms_ref[...] = jnp.sqrt(totals / count + 1e-06)

    for g in range(group):
        for b in range(full // LANES):
            out_ref[g, b * LANES : (b + 1) * LANES, :] = main_ref[g, :, b * LANES : (b + 1) * LANES].T
        start = pl.multiple_of((step * group + g) * rest, 8)
        out_ref[g, full:, :] = turned[pl.ds(start, rest), :]


def shards(n, half_integrals, pair_list, occupied_energy, virtual_orbitals, tile_order):
    pair_rows, columns, basis = half_integrals.shape
    virtuals = virtual_orbitals.shape[1]
    pairs = n * pair_rows
    span = columns // n
    deep = round_up(basis, LANES)
    broad = round_up(virtuals, LANES)
    full = virtuals // LANES * LANES
    rest = virtuals - full
    rows = span * pair_rows
    group = 4
    flops = 6 * pair_rows * columns * basis * virtuals
    vmem = pl.BlockSpec(memory_space=pltpu.VMEM)
    anywhere = pl.BlockSpec(memory_space=pl.ANY)

    def whole(*shape):
        return pl.BlockSpec(shape, lambda i: (0,) * len(shape))

    tiles = LANES // TILE_S
    xs, w_high, w_low, scales = pl.pallas_call(
        prepare_kernel,
        grid=(columns // LANES,),
        out_shape=(
            jax.ShapeDtypeStruct((deep // LANES, columns * pair_rows, LANES), jnp.float32),
            jax.ShapeDtypeStruct((deep, broad), jnp.bfloat16),
            jax.ShapeDtypeStruct((deep, broad), jnp.bfloat16),
            jax.ShapeDtypeStruct((pair_rows, broad), jnp.float32),
        ),
        in_specs=[
            pl.BlockSpec(memory_space=pltpu.SMEM),
            whole(2, pairs),
            whole(1, occupied_energy.shape[0]),
            pl.BlockSpec((pair_rows, basis, LANES), lambda i: (0, 0, i)),
            whole(basis, virtuals),
        ],
        out_specs=(anywhere, whole(deep, broad), whole(deep, broad), whole(pair_rows, broad)),
        scratch_shapes=[
            pltpu.VMEM((pairs, LANES), jnp.float32),
            pltpu.VMEM((2, deep // LANES, LANES * pair_rows, LANES), jnp.float32),
            pltpu.SMEM(tile_order.shape, jnp.int32),
            pltpu.SemaphoreType.DMA((2, tiles)),
        ],
        compiler_params=pltpu.CompilerParams(vmem_limit_bytes=28 * 1024 * 1024),
        name="prepare",
    )(tile_order, pair_list.T, occupied_energy.reshape(1, -1), pltpu.with_memory_space_constraint(jnp.swapaxes(half_integrals, 1, 2), pltpu.HBM), virtual_orbitals)
    recv_main, recv_rest, sq_recv = pl.pallas_call(
        functools.partial(exchange_kernel, n),
        out_shape=(
            jax.ShapeDtypeStruct((span, pairs, full), jnp.float32),
            jax.ShapeDtypeStruct((pairs, span * rest), jnp.float32),
            jax.ShapeDtypeStruct((n, pair_rows, LANES), jnp.float32),
        ),
        in_specs=[anywhere, vmem, vmem, vmem],
        out_specs=(anywhere, anywhere, anywhere),
        scratch_shapes=[
            pltpu.VMEM((2, deep // LANES, rows, LANES), jnp.float32),
            pltpu.VMEM((rows, deep), jnp.bfloat16),
            pltpu.VMEM((rows, deep), jnp.bfloat16),
            pltpu.VMEM((pair_rows, broad), jnp.float32),
            pltpu.VMEM((pair_rows, LANES), jnp.float32),
            pltpu.VMEM((n, span, pair_rows, full), jnp.float32),
            pltpu.VMEM((n, pair_rows, span * rest), jnp.float32),
            pltpu.SemaphoreType.DMA((2,)),
            pltpu.SemaphoreType.DMA((n,)),
            pltpu.SemaphoreType.DMA((n,)),
            pltpu.SemaphoreType.DMA((n,)),
            pltpu.SemaphoreType.DMA((n,)),
            pltpu.SemaphoreType.DMA((n,)),
            pltpu.SemaphoreType.DMA((n,)),
            pltpu.SemaphoreType.DMA((3,)),
        ],
        compiler_params=pltpu.CompilerParams(
            collective_id=0, has_side_effects=True, vmem_limit_bytes=20 * 1024 * 1024
        ),
        cost_estimate=pl.CostEstimate(flops=flops, bytes_accessed=4 * half_integrals.size, transcendentals=0),
        name="exchange",
    )(xs, w_high, w_low, scales)
    out, rms = pl.pallas_call(
        functools.partial(unpack_kernel, columns * virtuals),
        grid=(span // group,),
        out_shape=(
            jax.ShapeDtypeStruct((span, virtuals, pairs), jnp.float32),
            jax.ShapeDtypeStruct((1, pairs), jnp.float32),
        ),
        in_specs=[
            pl.BlockSpec((group, pairs, full), lambda i: (i, 0, 0)),
            pl.BlockSpec((pairs, span * rest), lambda i: (0, 0)),
            pl.BlockSpec((pairs, LANES), lambda i: (0, 0)),
        ],
        out_specs=(
            pl.BlockSpec((group, virtuals, pairs), lambda i: (i, 0, 0)),
            pl.BlockSpec((1, pairs), lambda i: (0, 0)),
        ),
        scratch_shapes=[pltpu.VMEM((span * rest, pairs), jnp.float32)],
        compiler_params=pltpu.CompilerParams(vmem_limit_bytes=20 * 1024 * 1024),
        name="unpack",
    )(recv_main, recv_rest, sq_recv.reshape(pairs, LANES))
    return (jnp.transpose(out, (2, 0, 1)), rms.reshape(-1))


def solution(mesh):
    in_specs = (
        P(("groups", "wide"), None, None),
        P("groups", None),
        P("groups"),
        P("groups", None),
        P(),
    )
    out_specs = (P("groups", "wide", None), P("groups"))
    return jax.shard_map(
        functools.partial(shards, mesh.shape["wide"]),
        mesh=mesh, in_specs=in_specs, out_specs=out_specs, check_vma=False,
    )
```
